16 devices in a mesh: dp: 1, tp: 16 (over x, y, z, core).
Axes of the slice: x: 2, y: 2, z: 2, core: 2. Of those that a mesh axis runs over, the one named last changes fastest.
Arguments:
- x: bfloat16 [2048, 3584], P('dp')
- dy: bfloat16 [2048, 3584], P('dp')
- gate: bfloat16 [2048, 14336], P('dp', 'tp')
- up: bfloat16 [2048, 14336], P('dp', 'tp')
- w_gate: bfloat16 [3584, 14336], P(None, 'tp')
- w_up: bfloat16 [3584, 14336], P(None, 'tp')
- w_down: bfloat16 [14336, 3584], P('tp')
Outputs:
- output 1: bfloat16 [2048, 3584], P('dp')
- output 2: bfloat16 [3584, 14336], P('dp', 'tp')
- output 3: bfloat16 [3584, 14336], P('dp', 'tp')
- output 4: bfloat16 [14336, 3584], P(('dp', 'tp'))
All inputs are finite; a program needn't handle non-finite values.
Results may differ from the reference program's by a relative error of at most 0.012.
Values are sent between devices in bfloat16 or wider.
A program may use at most 2 GiB of HBM per device.

```python
import jax
import jax.numpy as jnp

ROWS = 2048
D = 3584
FF = 14336


def act(gate, up):
    return jax.nn.gelu(gate) * up


def setup_inputs(seed: int = 0, part: int = 0) -> dict:
    kx, ky, ka, kb, kg, ku, kd = jax.random.split(jax.random.key(seed), 7)
    kx, ky, ka, kb = (jax.random.fold_in(k, part) for k in (kx, ky, ka, kb))
    drawn = {
        "x": jax.random.normal(kx, (ROWS, D), jnp.float32),
        "dy": jax.random.normal(ky, (ROWS, D), jnp.float32),
        "gate": jax.random.normal(ka, (ROWS, FF), jnp.float32),
        "up": jax.random.normal(kb, (ROWS, FF), jnp.float32),
        "w_gate": jax.random.normal(kg, (D, FF), jnp.float32) * D**-0.5,
        "w_up": jax.random.normal(ku, (D, FF), jnp.float32) * D**-0.5,
        "w_down": jax.random.normal(kd, (FF, D), jnp.float32) * FF**-0.5,
    }
    return {k: v.astype(jnp.bfloat16) for k, v in drawn.items()}


def reference(x, dy, gate, up, w_gate, w_up, w_down):
    hidden, back = jax.vjp(act, gate.astype(jnp.float32), up.astype(jnp.float32))
    d_hidden = jnp.dot(dy, w_down.T, preferred_element_type=jnp.float32)
    d_gate, d_up = (g.astype(jnp.bfloat16) for g in back(d_hidden))
    dx = jnp.dot(d_gate, w_gate.T, preferred_element_type=jnp.float32) + jnp.dot(d_up, w_up.T, preferred_element_type=jnp.float32)
    dw_gate = jnp.dot(x.T, d_gate, preferred_element_type=jnp.float32)
    dw_up = jnp.dot(x.T, d_up, preferred_element_type=jnp.float32)
    dw_down = jnp.dot(hidden.astype(jnp.bfloat16).T, dy, preferred_element_type=jnp.float32)
    return tuple(g.astype(jnp.bfloat16) for g in (dx, dw_gate, dw_up, dw_down))
```

```python
import functools

import jax
import jax.numpy as jnp
from jax import lax
from jax.experimental import pallas as pl
from jax.experimental.pallas import tpu as pltpu
from jax.sharding import PartitionSpec as P

MESH = pl.DeviceIdType.MESH
BF, F32 = jnp.bfloat16, jnp.float32
CHUNK = 256
HALF = CHUNK // 2
TILE = 256
C0 = 0.7978845608028654
C1 = 0.044715
STRIDES = (8, 4, 2)
ORDERS = ((0, 1, 2), (1, 2, 0), (2, 0, 1))
NT = (((1,), (1,)), ((), ()))
TN = (((0,), (0,)), ((), ()))
NN = (((1,), (0,)), ((), ()))
D, RS1, RS2, RS3, AG3, AG2, AG1, DG = range(8)
ROWS_OF = (HALF, HALF // 2, HALF // 4, HALF // 8, HALF // 8, HALF // 4, HALF // 2, HALF)

EVENTS1 = {1: ((1, 1), (3, 3)), 2: ((7, 6), (6, 5)), 3: ((2, 2), (5, 4)), 5: ((4, 3),)}
EVENTS2 = {1: ((1, 1), (3, 3)), 2: ((7, 6), (6, 5)), 3: ((2, 2), (5, 4)), 4: ((4, 3),)}
LAST_LAG = 6


def kernel(x, dy, gate, up, w_gate, w_up, w_down, dx, dwg, dwu, dwd,
           wgu, wd, dgu, hidt, pbuf, own, summed, acc, r1, r2, r3,
           wsem, insem, colsem, outsem, lsem, ssem, rsem):
    rows, dim = x.shape
    ff = gate.shape[1]
    n_chunks = rows // CHUNK
    n_tiles = dim // TILE
    n_dx = 4
    dxw = dim // n_dx
    units = dim // 128
    w2 = units // 3
    w0 = units - 2 * w2
    parts = ((0, w0 * 128), (w0 * 128, w2 * 128), ((w0 + w2) * 128, w2 * 128))

    me = lax.axis_index("tp")
    core = me % 2
    bits = tuple((me // s) % 2 for s in STRIDES)
    near = tuple(me + s - 2 * s * b for s, b in zip(STRIDES, bits))
    partner = me + 1 - 2 * core

    def load_chunk(k, slot, dyb, gb, ub):
        r = pl.ds(pl.multiple_of(k * CHUNK, CHUNK), CHUNK)
        return (pltpu.make_async_copy(dy.at[r], dyb.at[slot], insem.at[0, slot]),
                pltpu.make_async_copy(gate.at[r], gb.at[slot], insem.at[1, slot]),
                pltpu.make_async_copy(up.at[r], ub.at[slot], insem.at[2, slot]))

    def load_col(t, q, xcol, dycol):
        c = pl.ds(pl.multiple_of(t * TILE, TILE), TILE)
        return (pltpu.make_async_copy(x.at[:, c], xcol.at[q], colsem.at[0, q]),
                pltpu.make_async_copy(dy.at[:, c], dycol.at[q], colsem.at[1, q]))

    wloads = (pltpu.make_async_copy(w_down, wd, wsem.at[0]),
              pltpu.make_async_copy(w_gate, wgu.at[:, 0:ff], wsem.at[1]),
              pltpu.make_async_copy(w_up, wgu.at[:, ff:2 * ff], wsem.at[2]))
    for c in wloads:
        c.start()

    barrier = pltpu.get_barrier_semaphore()
    for other in (*near, partner):
        pl.semaphore_signal(barrier, inc=1, device_id={"tp": other}, device_id_type=MESH)
    pl.semaphore_wait(barrier, 4)

    def send(src, dst, stage, k, to):
        pltpu.make_async_remote_copy(src_ref=src, dst_ref=dst, send_sem=ssem.at[stage, k], recv_sem=rsem.at[stage, k],
                                     device_id={"tp": to}, device_id_type=MESH).start()

    def await_bytes(stage, k, sems):
        ref = summed.at[0, 0:ROWS_OF[stage]]
        pltpu.make_async_copy(ref, ref, sems.at[stage, k]).wait()

    def geometry(p):
        c0, cw = parts[p]
        a, b, c = ORDERS[p]
        return slice(c0, c0 + cw), (bits[a], bits[b], bits[c]), (near[a], near[b], near[c])

    def at(o, n):
        return pl.ds(pl.multiple_of(o, HALF // 8), n)

    def stage0(k):
        send(pbuf.at[...], summed.at[k], D, k, partner)

    def stage1(k):
        await_bytes(D, k, ssem)
        await_bytes(D, k, rsem)
        h = HALF // 2
        a = lax.rem(k, 4)
        for p in range(3):
            cols, (b1, _, _), (to, _, _) = geometry(p)
            out, keep = at(h * (1 - b1), h), at(h * b1, h)
            summed[k, out, cols] = (own[out, cols] + summed[k, out, cols].astype(F32)).astype(BF)
            send(summed.at[k, out, cols], r1.at[k, :, cols], RS1, k, to)
            acc[a, :, cols] = own[keep, cols] + summed[k, keep, cols].astype(F32)

    def stage2(k):
        await_bytes(RS1, k, rsem)
        h = HALF // 4
        a = lax.rem(k, 4)
        for p in range(3):
            cols, (b1, b2, _), (_, to, _) = geometry(p)
            out, keep = at(h * (1 - b2), h), at(h * b2, h)
            stage = at(2 * h * b1 + h * (1 - b2), h)
            summed[k, stage, cols] = (acc[a, out, cols] + r1[k, out, cols].astype(F32)).astype(BF)
            send(summed.at[k, stage, cols], r2.at[k, :, cols], RS2, k, to)
            acc[a, keep, cols] = acc[a, keep, cols] + r1[k, keep, cols].astype(F32)

    def stage3(k):
        await_bytes(RS2, k, rsem)
        h = HALF // 8
        a = lax.rem(k, 4)
        for p in range(3):
            cols, (b1, b2, b3), (_, _, to) = geometry(p)
            out, keep = at(h * (1 - b3), h), at(h * b3, h)
            aout, akeep = at(2 * h * b2 + h * (1 - b3), h), at(2 * h * b2 + h * b3, h)
            stage = at(4 * h * b1 + 2 * h * b2 + h * (1 - b3), h)
            summed[k, stage, cols] = (acc[a, aout, cols] + r2[k, out, cols].astype(F32)).astype(BF)
            send(summed.at[k, stage, cols], r3.at[k, :, cols], RS3, k, to)
            acc[a, akeep, cols] = acc[a, akeep, cols] + r2[k, keep, cols].astype(F32)

    def stage4(k):
        await_bytes(RS3, k, rsem)
        h = HALF // 8
        a = lax.rem(k, 4)
        for p in range(3):
            cols, (b1, b2, b3), (_, _, to) = geometry(p)
            akeep = at(2 * h * b2 + h * b3, h)
            o = 4 * h * b1 + 2 * h * b2 + h * b3
            mine = at(o, h)
            place = at(k * CHUNK + core * HALF + o, h)
            summed[k, mine, cols] = (acc[a, akeep, cols] + r3[k, :, cols].astype(F32)).astype(BF)
            send(summed.at[k, mine, cols], dx.at[place, cols], AG3, k, to)
            pltpu.make_async_copy(summed.at[k, mine, cols], dx.at[place, cols], lsem.at[k]).start()

    def gather(k, got, stage, span, which):
        await_bytes(got, k, rsem)
        for p in range(3):
            cols, (b1, b2, _), tos = geometry(p)
            o = (HALF // 2) * b1 + (HALF // 4) * b2 if which == 1 else (HALF // 2) * b1
            place = at(k * CHUNK + core * HALF + o, span)
            send(dx.at[place, cols], dx.at[place, cols], stage, k, tos[which])

    def stage5(k):
        ref = summed.at[0, 0:HALF // 8]
        pltpu.make_async_copy(ref, ref, lsem.at[k]).wait()
        gather(k, AG3, AG2, HALF // 4, 1)

    def stage6(k):
        gather(k, AG2, AG1, HALF // 2, 0)

    def stage7(k):
        await_bytes(AG1, k, rsem)
        place = at(k * CHUNK + core * HALF, HALF)
        send(dx.at[place], dx.at[place], DG, k, partner)

    stages = (stage0, stage1, stage2, stage3, stage4, stage5, stage6, stage7)

    def run(table, s, j):
        for stage, lag in table.get(j, ()):
            k = s - lag

            @pl.when(jnp.logical_and(k >= 0, k < n_chunks))
            def _():
                stages[stage](k)

    def slot1(bufs, s):
        dyb, gb, ub = bufs
        q = lax.rem(s, 2)

        @pl.when(s + 1 < n_chunks)
        def _():
            for c in load_chunk(s + 1, 1 - q, *bufs):
                c.start()

        for c in load_chunk(s, q, *bufs):
            c.wait()

        @pl.when(s == 0)
        def _():
            wloads[0].wait()

        base = pl.multiple_of(s * CHUNK, CHUNK)
        dh = lax.dot_general(dyb[q], wd[...], NT, preferred_element_type=F32)
        g, u = gb[q].astype(F32), ub[q].astype(F32)
        g2 = g * g
        t = jnp.tanh((C0 * g) * (1.0 + C1 * g2))
        cdf = 0.5 + 0.5 * t
        gelu = g * cdf
        slope = cdf + g * (cdf * (1.0 - t)) * (C0 + (3.0 * C0 * C1) * g2)
        hidt[:, pl.ds(base, CHUNK)] = (gelu * u).astype(BF).T
        dgu[pl.ds(base, CHUNK), 0:ff] = (dh * u * slope).astype(BF)
        dgu[pl.ds(base, CHUNK), ff:2 * ff] = (dh * gelu).astype(BF)

        @pl.when(s == 0)
        def _():
            wloads[1].wait()
            wloads[2].wait()

        run(EVENTS1, s, 1)
        theirs = pl.ds(pl.multiple_of(base + HALF * (1 - core), HALF), HALF)
        mine = pl.ds(pl.multiple_of(base + HALF * core, HALF), HALF)
        for n in range(n_dx):
            cols = slice(n * dxw, (n + 1) * dxw)
            lhs = jnp.concatenate([dgu[theirs], dgu[mine]], axis=0)
            term = lax.dot_general(lhs, wgu[cols], NT, preferred_element_type=F32)
            pbuf[:, cols] = term[:HALF].astype(BF)
            own[:, cols] = term[HALF:]
            if n == n_dx - 1:
                stage0(s)
            run(EVENTS1, s, n + 2)

    def phase1(*bufs):
        for c in load_chunk(0, 0, *bufs):
            c.start()

        def body(s, _):
            slot1(bufs, s)
            return ()

        lax.fori_loop(0, n_chunks, body, ())

    pl.run_scoped(phase1, pltpu.VMEM((2, CHUNK, dim), BF), pltpu.VMEM((2, CHUNK, ff), BF), pltpu.VMEM((2, CHUNK, ff), BF))

    def put(t, q, outg, outd):
        r = pl.ds(pl.multiple_of(t * TILE, TILE), TILE)
        return (pltpu.make_async_copy(outg.at[q, :, 0:ff], dwg.at[r], outsem.at[0, q]),
                pltpu.make_async_copy(outg.at[q, :, ff:2 * ff], dwu.at[r], outsem.at[1, q]),
                pltpu.make_async_copy(outd.at[q], dwd.at[:, r], outsem.at[2, q]))

    def slot2(bufs, i):
        xcol, dycol, outg, outd = bufs
        s = n_chunks + i
        for q in range(2):
            tile = 2 * i + q
            loads, puts = load_col(tile, q, xcol, dycol), put(tile, q, outg, outd)
            for c in loads:
                c.wait()

            @pl.when(i > 0)
            def _():
                for c in puts:
                    c.wait()

            outg[q] = lax.dot_general(xcol[q], dgu[...], TN, preferred_element_type=F32).astype(BF)
            puts[0].start()
            puts[1].start()
            run(EVENTS2, s, 2 * q + 1)
            outd[q] = lax.dot_general(hidt[...], dycol[q], NN, preferred_element_type=F32).astype(BF)
            puts[2].start()

            @pl.when(tile + 2 < n_tiles)
            def _():
                for c in load_col(tile + 2, q, xcol, dycol):
                    c.start()

            run(EVENTS2, s, 2 * q + 2)

    n_slots = n_tiles // 2

    def phase2(*bufs):
        for q in range(2):
            for c in load_col(q, q, *bufs[:2]):
                c.start()

        def body(i, _):
            slot2(bufs, i)
            return ()

        lax.fori_loop(0, n_slots, body, ())
        for q in range(2):
            for c in put(0, q, *bufs[2:]):
                c.wait()

    pl.run_scoped(phase2, pltpu.VMEM((2, rows, TILE), BF), pltpu.VMEM((2, rows, TILE), BF),
                  pltpu.VMEM((2, TILE, 2 * ff), BF), pltpu.VMEM((2, ff, TILE), BF))

    def slot3(s, _):
        for j in range(1, 6):
            run(EVENTS1, s, j)
        return ()

    lax.fori_loop(n_chunks + n_slots, max(n_chunks + n_slots, n_chunks + LAST_LAG), slot3, ())

    def finish(k, _):
        await_bytes(DG, k, rsem)
        for stage in range(RS1, DG + 1):
            await_bytes(stage, k, ssem)
        return ()

    lax.fori_loop(0, n_chunks, finish, ())


def backward(x, dy, gate, up, w_gate, w_up, w_down):
    rows, dim = x.shape
    ff = gate.shape[1]
    n_chunks = rows // CHUNK
    anyspec = pl.BlockSpec(memory_space=pl.ANY)
    vmem = pltpu.VMEM
    return pl.pallas_call(
        kernel,
        out_shape=(jax.ShapeDtypeStruct((rows, dim), BF), jax.ShapeDtypeStruct((dim, ff), BF),
                   jax.ShapeDtypeStruct((dim, ff), BF), jax.ShapeDtypeStruct((ff, dim), BF)),
        in_specs=[anyspec] * 7,
        out_specs=(anyspec,) * 4,
        scratch_shapes=[
            vmem((dim, 2 * ff), BF), vmem((ff, dim), BF), vmem((rows, 2 * ff), BF), vmem((ff, rows), BF),
            vmem((HALF, dim), BF), vmem((HALF, dim), F32), vmem((n_chunks, HALF, dim), BF), vmem((4, HALF // 2, dim), F32),
            vmem((n_chunks, HALF // 2, dim), BF), vmem((n_chunks, HALF // 4, dim), BF), vmem((n_chunks, HALF // 8, dim), BF),
            pltpu.SemaphoreType.DMA((3,)), pltpu.SemaphoreType.DMA((3, 2)), pltpu.SemaphoreType.DMA((2, 2)),
            pltpu.SemaphoreType.DMA((3, 2)), pltpu.SemaphoreType.DMA((n_chunks,)),
            pltpu.SemaphoreType.DMA((8, n_chunks)), pltpu.SemaphoreType.DMA((8, n_chunks)),
        ],
        compiler_params=pltpu.CompilerParams(collective_id=0, has_side_effects=True, vmem_limit_bytes=67_000_000),
        name="mlp_backward",
    )(x, dy, gate, up, w_gate, w_up, w_down)


def solution(mesh):
    tokens, columns, rows = P("dp", None), P(None, "tp"), P("tp", None)
    return jax.shard_map(
        backward,
        mesh=mesh,
        in_specs=(tokens, tokens, P("dp", "tp"), P("dp", "tp"), columns, columns, rows),
        out_specs=(tokens, P("dp", "tp"), P("dp", "tp"), P(("dp", "tp"), None)),
        check_vma=False,
    )
```

```python
import functools

import jax
import jax.numpy as jnp
from jax import lax
from jax.experimental import pallas as pl
from jax.experimental.pallas import tpu as pltpu
from jax.sharding import PartitionSpec as P

MESH = pl.DeviceIdType.MESH
BF, F32 = jnp.bfloat16, jnp.float32
CHUNK = 256
HALF = CHUNK // 2
SLOTS = 4
VMEM_LIMIT, WRITER_LIMIT = 32_000_000, 1_000_000
TILE = 256
C0 = 0.7978845608028654
C1 = 0.044715
STRIDES = (8, 4, 2)
NT = (((1,), (1,)), ((), ()))
TN = (((0,), (0,)), ((), ()))
NN = (((1,), (0,)), ((), ()))
D, RS1, RS2, RS3, AG3, AG2, AG1, DG = range(8)
ROWS_OF = (HALF, HALF // 2, HALF // 4, HALF // 8, HALF // 8, HALF // 4, HALF // 2, HALF)

POINTS = (
    (2, 4, 6, 8, 10, 12, 14, 16),
    (4, 7, 8, 11, 12, 15, 18, 19),
    (6, 9, 10, 14, 17, 18, 20, 21),
    (7, 11, 12, 16, 20, 21, 22, 23),
    (9, 13, 14, 18, 22, 23, 24, 25),
    (11, 20, 22, 25, 26, 27, 28, 30),
    (14, 23, 25, 28, 29, 31, 32, 33),
)
PRIO = (4, 3, 2, 5, 1, 7, 6)


def kernel(x, dy, gate, up, w_gate, w_up, w_down, kept, dgu, hidt, pbuf, own, staged, acc,
           wsem, insem, colsem, credit, ssem, rsem):
    rows, dim = x.shape
    ff = gate.shape[1]
    n_chunks = rows // CHUNK
    n_tiles = dim // TILE
    n_blocks = dim // ff
    down = slice(rows, rows + ff)
    starts = (rows + ff, rows + 2 * ff)

    units = dim // 128
    w2 = units // 3
    w0 = units - 2 * w2
    parts = ((0, w0 * 128), (w0 * 128, w2 * 128), ((w0 + w2) * 128, w2 * 128))

    me = lax.axis_index("tp")
    core = me % 2
    bits = tuple((me // s) % 2 for s in STRIDES)
    near = tuple(me + s - 2 * s * b for s, b in zip(STRIDES, bits))
    partner = me + 1 - 2 * core

    def load_chunk(k, slot, dyb, gb, ub):
        r = pl.ds(pl.multiple_of(k * CHUNK, CHUNK), CHUNK)
        return (pltpu.make_async_copy(dy.at[r], dyb.at[slot], insem.at[0, slot]),
                pltpu.make_async_copy(gate.at[r], gb.at[slot], insem.at[1, slot]),
                pltpu.make_async_copy(up.at[r], ub.at[slot], insem.at[2, slot]))

    def load_col(t, q, xcol, dycol):
        c = pl.ds(pl.multiple_of(t * TILE, TILE), TILE)
        return (pltpu.make_async_copy(x.at[:, c], xcol.at[q], colsem.at[0, q]),
                pltpu.make_async_copy(dy.at[:, c], dycol.at[q], colsem.at[1, q]))

    def block(w, b):
        return slice(starts[w], starts[w] + ff), slice(b * ff, (b + 1) * ff)

    def weight(w, lo, hi):
        pieces = []
        while lo < hi:
            b = lo // ff
            end = min(hi, (b + 1) * ff)
            pieces.append(kept[starts[w] + lo - b * ff:starts[w] + end - b * ff, b * ff:(b + 1) * ff])
            lo = end
        return jnp.concatenate(pieces, axis=0)

    download = pltpu.make_async_copy(w_down, kept.at[down], wsem.at[2 * n_blocks])
    wloads = tuple(tuple(pltpu.make_async_copy(src.at[b * ff:(b + 1) * ff], kept.at[block(w, b)], wsem.at[2 * b + w])
                         for w, src in enumerate((w_gate, w_up))) for b in range(n_blocks))
    download.start()

    barrier = pltpu.get_barrier_semaphore()
    for other in (*near, partner):
        pl.semaphore_signal(barrier, inc=1, device_id={"tp": other}, device_id_type=MESH)
    pl.semaphore_wait(barrier, 4)

    def send(src, dst, stage, k, to):
        pltpu.make_async_remote_copy(src_ref=src, dst_ref=dst, send_sem=ssem.at[stage, k], recv_sem=rsem.at[stage, k],
                                     device_id={"tp": to}, device_id_type=MESH).start()

    def await_bytes(stage, k, sems):
        ref = kept.at[0:ROWS_OF[stage]]
        pltpu.make_async_copy(ref, ref, sems.at[stage, k]).wait()

    def pick(values, i):
        return jnp.where(i == 0, values[0], jnp.where(i == 1, values[1], values[2]))

    def geometry(p, k):
        c0, cw = parts[p]
        dims = [lax.rem(p + k + i, 3) for i in range(3)]
        return slice(c0, c0 + cw), [pick(bits, d) for d in dims], [pick(near, d) for d in dims]

    def at(o, n):
        return pl.ds(pl.multiple_of(o, HALF // 8), n)

    def mine_at(k, o, n):
        return at(k * CHUNK + HALF * core + o, n)

    def spare_at(k, o, n):
        return at(k * CHUNK + HALF * (1 - core) + o, n)

    def stage0(k):
        send(pbuf, kept.at[spare_at(k, 0, HALF)], D, k, partner)

    q1, q2, q3 = HALF // 2, HALF // 4, HALF // 8

    def stage1(k):
        await_bytes(D, k, ssem)
        await_bytes(D, k, rsem)

        @pl.when(k >= SLOTS)
        def _():
            for stage in (RS1, RS2, RS3):
                await_bytes(stage, k - SLOTS, ssem)

        a = lax.rem(k, SLOTS)
        for p in range(3):
            cols, (b1, _, _), (to, _, _) = geometry(p, k)
            out, keep = q1 * (1 - b1), q1 * b1
            staged[a, 0:q1, cols] = (own[at(out, q1), cols] + kept[mine_at(k, out, q1), cols].astype(F32)).astype(BF)
            send(staged.at[a, 0:q1, cols], kept.at[spare_at(k, 0, q1), cols], RS1, k, to)
            acc[a, :, cols] = own[at(keep, q1), cols] + kept[mine_at(k, keep, q1), cols].astype(F32)

    def stage2(k):
        await_bytes(RS1, k, rsem)
        a = lax.rem(k, SLOTS)
        for p in range(3):
            cols, (_, b2, _), (_, to, _) = geometry(p, k)
            out, keep = q2 * (1 - b2), q2 * b2
            stage = slice(q1, q1 + q2)
            staged[a, stage, cols] = (acc[a, at(out, q2), cols] + kept[spare_at(k, out, q2), cols].astype(F32)).astype(BF)
            send(staged.at[a, stage, cols], kept.at[spare_at(k, q1, q2), cols], RS2, k, to)
            acc[a, at(keep, q2), cols] = acc[a, at(keep, q2), cols] + kept[spare_at(k, keep, q2), cols].astype(F32)

    def stage3(k):
        await_bytes(RS2, k, rsem)
        a = lax.rem(k, SLOTS)
        for p in range(3):
            cols, (_, b2, b3), (_, _, to) = geometry(p, k)
            out, keep = q3 * (1 - b3), q3 * b3
            stage = slice(q1 + q2, q1 + q2 + q3)
            staged[a, stage, cols] = (acc[a, at(q2 * b2 + out, q3), cols]
                                      + kept[spare_at(k, q1 + out, q3), cols].astype(F32)).astype(BF)
            send(staged.at[a, stage, cols], kept.at[spare_at(k, q1 + q2, q3), cols], RS3, k, to)
            place = at(q2 * b2 + keep, q3)
            acc[a, place, cols] = acc[a, place, cols] + kept[spare_at(k, q1 + keep, q3), cols].astype(F32)

    def stage4(k):
        await_bytes(RS3, k, rsem)
        a = lax.rem(k, SLOTS)
        for p in range(3):
            cols, (b1, b2, b3), (_, _, to) = geometry(p, k)
            place = mine_at(k, q1 * b1 + q2 * b2 + q3 * b3, q3)
            kept[place, cols] = (acc[a, at(q2 * b2 + q3 * b3, q3), cols]
                                 + kept[spare_at(k, q1 + q2, q3), cols].astype(F32)).astype(BF)
            send(kept.at[place, cols], kept.at[place, cols], AG3, k, to)
        pl.semaphore_signal(credit, inc=1, device_id={"tp": partner}, device_id_type=MESH)

    def gather(k, got, stage, span, which):
        await_bytes(got, k, rsem)
        for p in range(3):
            cols, (b1, b2, _), tos = geometry(p, k)
            place = mine_at(k, q1 * b1 + q2 * b2 if which == 1 else q1 * b1, span)
            send(kept.at[place, cols], kept.at[place, cols], stage, k, tos[which])

    def stage5(k):
        gather(k, AG3, AG2, q2, 1)

    def stage6(k):
        gather(k, AG2, AG1, q1, 0)

    def stage7(k):
        await_bytes(AG1, k, rsem)
        pl.semaphore_wait(credit, 1)
        place = mine_at(k, 0, HALF)
        send(kept.at[place], kept.at[place], DG, k, partner)

    stages = (stage0, stage1, stage2, stage3, stage4, stage5, stage6, stage7)

    def run(base, n, per, i, j):
        for stage in PRIO:
            turns = [(k, (p - base) // per) for k, p in enumerate(POINTS[stage - 1])
                     if base <= p < base + n * per and (p - base) % per == j]
            if turns:
                k = sum(jnp.where(i == t, k, 0) for k, t in turns)
                now = functools.reduce(jnp.logical_or, [i == t for _, t in turns])

                @pl.when(now)
                def _():
                    stages[stage](k)

    def slot1(bufs, s):
        dyb, gb, ub = bufs
        q = lax.rem(s, 2)

        @pl.when(s + 1 < n_chunks)
        def _():
            for c in load_chunk(s + 1, 1 - q, *bufs):
                c.start()

        @pl.when(s == 0)
        def _():
            download.wait()
            for pair in wloads:
                for c in pair:
                    c.start()

        for c in load_chunk(s, q, *bufs):
            c.wait()

        base = pl.multiple_of(s * CHUNK, CHUNK)
        dh = lax.dot_general(dyb[q], kept[down], NT, preferred_element_type=F32)
        g, u = gb[q].astype(F32), ub[q].astype(F32)
        g2 = g * g
        t = jnp.tanh((C0 * g) * (1.0 + C1 * g2))
        cdf = 0.5 + 0.5 * t
        gelu = g * cdf
        slope = cdf + g * (cdf * (1.0 - t)) * (C0 + (3.0 * C0 * C1) * g2)
        hidt[:, pl.ds(base, CHUNK)] = (gelu * u).astype(BF).T
        dgu[pl.ds(base, CHUNK), 0:ff] = (dh * u * slope).astype(BF)
        dgu[pl.ds(base, CHUNK), ff:2 * ff] = (dh * gelu).astype(BF)

        @pl.when(s == 0)
        def _():
            for pair in wloads:
                for c in pair:
                    c.wait()

        run(0, n_chunks, 2, s, 0)
        theirs = pl.ds(pl.multiple_of(base + HALF * (1 - core), HALF), HALF)
        mine = pl.ds(pl.multiple_of(base + HALF * core, HALF), HALF)
        lhs = jnp.concatenate([dgu[theirs], dgu[mine]], axis=0)
        for n in range(2):
            cols = slice(n * (dim // 2), (n + 1) * (dim // 2))
            rhs = jnp.concatenate([weight(w, cols.start, cols.stop) for w in range(2)], axis=1)
            term = lax.dot_general(lhs, rhs, NT, preferred_element_type=F32)
            pbuf[:, cols] = term[:HALF].astype(BF)
            own[:, cols] = term[HALF:]
        stage0(s)
        run(0, n_chunks, 2, s, 1)

    def phase1(*bufs):
        for c in load_chunk(0, 0, *bufs):
            c.start()

        def body(s, _):
            slot1(bufs, s)
            return ()

        lax.fori_loop(0, n_chunks, body, ())

    pl.run_scoped(phase1, pltpu.VMEM((2, CHUNK, dim), BF), pltpu.VMEM((2, CHUNK, ff), BF), pltpu.VMEM((2, CHUNK, ff), BF))

    base2 = n_chunks * 2

    def slot2(bufs, t):
        q = lax.rem(t, 3)

        @pl.when(t + 2 < n_tiles)
        def _():
            for c in load_col(t + 2, lax.rem(t + 2, 3), *bufs):
                c.start()

        xcol, dycol = bufs
        loads = load_col(t, q, *bufs)
        r = pl.ds(pl.multiple_of(t * TILE, TILE), TILE)
        loads[0].wait()
        loads[1].wait()
        dw = lax.dot_general(xcol[q], dgu[...], TN, preferred_element_type=F32)
        dw = dw.astype(BF)
        for i in range(TILE // 128):
            row = t * TILE + i * 128
            lanes = pl.ds(pl.multiple_of((row // ff) * ff, 128), ff)
            for w in range(2):
                place = pl.ds(pl.multiple_of(starts[w] + row % ff, 128), 128)
                kept[place, lanes] = dw[i * 128:(i + 1) * 128, w * ff:(w + 1) * ff]
        kept[down, r] = lax.dot_general(hidt[...], dycol[q], NN, preferred_element_type=F32).astype(BF)
        run(base2, n_tiles, 1, t, 0)

    def phase2(*bufs):
        for t in range(2):
            for c in load_col(t, t, *bufs):
                c.start()

        def body(t, _):
            slot2(bufs, t)
            return ()

        lax.fori_loop(0, n_tiles, body, ())

    pl.run_scoped(phase2, pltpu.VMEM((3, rows, TILE), BF), pltpu.VMEM((3, rows, TILE), BF))

    rest = sorted((p, PRIO.index(stage), stage, k) for stage in range(1, 8) for k, p in enumerate(POINTS[stage - 1])
                  if p >= base2 + n_tiles)
    for _, _, stage, k in rest:
        stages[stage](k)

    def finish(k, _):
        await_bytes(DG, k, rsem)
        for stage in (AG3, AG2, AG1, DG):
            await_bytes(stage, k, ssem)

        @pl.when(k >= n_chunks - SLOTS)
        def _():
            for stage in (RS1, RS2, RS3):
                await_bytes(stage, k, ssem)

        return ()

    lax.fori_loop(0, n_chunks, finish, ())


def writer(kept, dx, dwg, dwu, dwd, sem):
    rows, (dim, ff) = dx.shape[0], dwg.shape
    pairs = [(kept.at[0:rows], dx), (kept.at[rows:rows + ff], dwd)]
    for w, out in enumerate((dwg, dwu)):
        start = rows + (1 + w) * ff
        pairs += [(kept.at[start:start + ff, b * ff:(b + 1) * ff], out.at[b * ff:(b + 1) * ff]) for b in range(dim // ff)]
    copies = [pltpu.make_async_copy(a, b, sem.at[i]) for i, (a, b) in enumerate(pairs)]
    for c in copies:
        c.start()
    for c in copies:
        c.wait()


def backward(x, dy, gate, up, w_gate, w_up, w_down):
    rows, dim = x.shape
    ff = gate.shape[1]
    n_chunks, n_blocks = rows // CHUNK, dim // ff
    hbm, inside = pl.BlockSpec(memory_space=pl.ANY), pl.BlockSpec(memory_space=pltpu.VMEM)
    vmem, dma = pltpu.VMEM, pltpu.SemaphoreType.DMA
    kept = pl.pallas_call(
        kernel,
        out_shape=vmem((rows + 3 * ff, dim), BF),
        in_specs=[hbm] * 7,
        out_specs=inside,
        scratch_shapes=[
            vmem((rows, 2 * ff), BF), vmem((ff, rows), BF), vmem((HALF, dim), BF), vmem((HALF, dim), F32),
            vmem((SLOTS, HALF // 8 * 7, dim), BF), vmem((SLOTS, HALF // 2, dim), F32),
            dma((2 * n_blocks + 1,)), dma((3, 2)), dma((2, 3)), pltpu.SemaphoreType.REGULAR,
            dma((8, n_chunks)), dma((8, n_chunks)),
        ],
        compiler_params=pltpu.CompilerParams(collective_id=0, has_side_effects=True, vmem_limit_bytes=VMEM_LIMIT),
        name="mlp_backward",
    )(x, dy, gate, up, w_gate, w_up, w_down)
    return pl.pallas_call(
        writer,
        out_shape=tuple(jax.ShapeDtypeStruct(g, BF) for g in ((rows, dim), (dim, ff), (dim, ff), (ff, dim))),
        in_specs=[inside],
        out_specs=(hbm,) * 4,
        scratch_shapes=[dma((2 * n_blocks + 2,))],
        compiler_params=pltpu.CompilerParams(vmem_limit_bytes=WRITER_LIMIT),
        name="writer",
    )(kept)


def solution(mesh):
    tokens, columns, rows = P("dp", None), P(None, "tp"), P("tp", None)
    return jax.shard_map(
        backward,
        mesh=mesh,
        in_specs=(tokens, tokens, P("dp", "tp"), P("dp", "tp"), columns, columns, rows),
        out_specs=(tokens, P("dp", "tp"), P("dp", "tp"), P(("dp", "tp"), None)),
        check_vma=False,
    )
```

```python
import functools

import jax
import jax.numpy as jnp
from jax import lax
from jax.experimental import pallas as pl
from jax.experimental.pallas import tpu as pltpu
from jax.sharding import PartitionSpec as P

MESH = pl.DeviceIdType.MESH
BF, F32 = jnp.bfloat16, jnp.float32
CHUNK = 256
HALF = CHUNK // 2
SLOTS = 4
VMEM_LIMIT, WRITER_LIMIT = 32_000_000, 1_000_000
TILE = 256
C0 = 0.7978845608028654
C1 = 0.044715
STRIDES = (8, 4, 2)
NT = (((1,), (1,)), ((), ()))
TN = (((0,), (0,)), ((), ()))
NN = (((1,), (0,)), ((), ()))
D, RS1, RS2, RS3, AG3, AG2, AG1, DG = range(8)
ROWS_OF = (HALF, HALF // 2, HALF // 4, HALF // 8, HALF // 8, HALF // 4, HALF // 2, HALF)

POINTS = (
    (2, 4, 6, 8, 10, 12, 14, 16),
    (4, 7, 8, 11, 12, 15, 18, 19),
    (6, 9, 10, 14, 17, 18, 20, 21),
    (7, 11, 12, 16, 20, 21, 22, 23),
    (9, 13, 14, 18, 22, 23, 24, 25),
    (11, 20, 22, 25, 26, 27, 28, 30),
    (14, 23, 25, 28, 29, 31, 32, 33),
)
PRIO = (4, 3, 2, 5, 1, 7, 6)


def kernel(x, dy, gate, up, w_gate, w_up, w_down, kept, dgu, hidt, pbuf, own, staged, acc,
           wsem, insem, colsem, credit, ssem, rsem):
    rows, dim = x.shape
    ff = gate.shape[1]
    n_chunks = rows // CHUNK
    n_tiles = dim // TILE
    n_blocks = dim // ff
    down = slice(rows, rows + ff)
    starts = (rows + ff, rows + 2 * ff)

    units = dim // 128
    w2 = units // 3
    w0 = units - 2 * w2
    parts = ((0, w0 * 128), (w0 * 128, w2 * 128), ((w0 + w2) * 128, w2 * 128))

    me = lax.axis_index("tp")
    core = me % 2
    bits = tuple((me // s) % 2 for s in STRIDES)
    near = tuple(me + s - 2 * s * b for s, b in zip(STRIDES, bits))
    partner = me + 1 - 2 * core

    def load_chunk(k, slot, dyb, gb, ub):
        r = pl.ds(pl.multiple_of(k * CHUNK, CHUNK), CHUNK)
        return (pltpu.make_async_copy(dy.at[r], dyb.at[slot], insem.at[0, slot]),
                pltpu.make_async_copy(gate.at[r], gb.at[slot], insem.at[1, slot]),
                pltpu.make_async_copy(up.at[r], ub.at[slot], insem.at[2, slot]))

    def load_col(t, q, xcol, dycol):
        c = pl.ds(pl.multiple_of(t * TILE, TILE), TILE)
        return (pltpu.make_async_copy(x.at[:, c], xcol.at[q], colsem.at[0, q]),
                pltpu.make_async_copy(dy.at[:, c], dycol.at[q], colsem.at[1, q]))

    def block(w, b):
        return slice(starts[w], starts[w] + ff), slice(b * ff, (b + 1) * ff)

    def weight(w, lo, hi):
        pieces = []
        while lo < hi:
            b = lo // ff
            end = min(hi, (b + 1) * ff)
            pieces.append(kept[starts[w] + lo - b * ff:starts[w] + end - b * ff, b * ff:(b + 1) * ff])
            lo = end
        return jnp.concatenate(pieces, axis=0)

    download = pltpu.make_async_copy(w_down, kept.at[down], wsem.at[2 * n_blocks])
    wloads = tuple(tuple(pltpu.make_async_copy(src.at[b * ff:(b + 1) * ff], kept.at[block(w, b)], wsem.at[2 * b + w])
                         for w, src in enumerate((w_gate, w_up))) for b in range(n_blocks))
    download.start()

    barrier = pltpu.get_barrier_semaphore()
    for other in (*near, partner):
        pl.semaphore_signal(barrier, inc=1, device_id={"tp": other}, device_id_type=MESH)

    def send(src, dst, stage, k, to):
        pltpu.make_async_remote_copy(src_ref=src, dst_ref=dst, send_sem=ssem.at[stage, k], recv_sem=rsem.at[stage, k],
                                     device_id={"tp": to}, device_id_type=MESH).start()

    def await_bytes(stage, k, sems):
        ref = kept.at[0:ROWS_OF[stage]]
        pltpu.make_async_copy(ref, ref, sems.at[stage, k]).wait()

    def pick(values, i):
        return jnp.where(i == 0, values[0], jnp.where(i == 1, values[1], values[2]))

    def geometry(p, k):
        c0, cw = parts[p]
        dims = [lax.rem(p + k + i, 3) for i in range(3)]
        return slice(c0, c0 + cw), [pick(bits, d) for d in dims], [pick(near, d) for d in dims]

    def at(o, n):
        return pl.ds(pl.multiple_of(o, HALF // 8), n)

    def mine_at(k, o, n):
        return at(k * CHUNK + HALF * core + o, n)

    def spare_at(k, o, n):
        return at(k * CHUNK + HALF * (1 - core) + o, n)

    def stage0(k):
        send(pbuf, kept.at[spare_at(k, 0, HALF)], D, k, partner)

    q1, q2, q3 = HALF // 2, HALF // 4, HALF // 8

    def stage1(k):
        await_bytes(D, k, ssem)
        await_bytes(D, k, rsem)

        @pl.when(k >= SLOTS)
        def _():
            for stage in (RS1, RS2, RS3):
                await_bytes(stage, k - SLOTS, ssem)

        a = lax.rem(k, SLOTS)
        for p in range(3):
            cols, (b1, _, _), (to, _, _) = geometry(p, k)
            out, keep = q1 * (1 - b1), q1 * b1
            staged[a, 0:q1, cols] = (own[at(out, q1), cols] + kept[mine_at(k, out, q1), cols].astype(F32)).astype(BF)
            send(staged.at[a, 0:q1, cols], kept.at[spare_at(k, 0, q1), cols], RS1, k, to)
            acc[a, :, cols] = own[at(keep, q1), cols] + kept[mine_at(k, keep, q1), cols].astype(F32)

    def stage2(k):
        await_bytes(RS1, k, rsem)
        a = lax.rem(k, SLOTS)
        for p in range(3):
            cols, (_, b2, _), (_, to, _) = geometry(p, k)
            out, keep = q2 * (1 - b2), q2 * b2
            stage = slice(q1, q1 + q2)
            staged[a, stage, cols] = (acc[a, at(out, q2), cols] + kept[spare_at(k, out, q2), cols].astype(F32)).astype(BF)
            send(staged.at[a, stage, cols], kept.at[spare_at(k, q1, q2), cols], RS2, k, to)
            acc[a, at(keep, q2), cols] = acc[a, at(keep, q2), cols] + kept[spare_at(k, keep, q2), cols].astype(F32)

    def stage3(k):
        await_bytes(RS2, k, rsem)
        a = lax.rem(k, SLOTS)
        for p in range(3):
            cols, (_, b2, b3), (_, _, to) = geometry(p, k)
            out, keep = q3 * (1 - b3), q3 * b3
            stage = slice(q1 + q2, q1 + q2 + q3)
            staged[a, stage, cols] = (acc[a, at(q2 * b2 + out, q3), cols]
                                      + kept[spare_at(k, q1 + out, q3), cols].astype(F32)).astype(BF)
            send(staged.at[a, stage, cols], kept.at[spare_at(k, q1 + q2, q3), cols], RS3, k, to)
            place = at(q2 * b2 + keep, q3)
            acc[a, place, cols] = acc[a, place, cols] + kept[spare_at(k, q1 + keep, q3), cols].astype(F32)

    def stage4(k):
        await_bytes(RS3, k, rsem)
        a = lax.rem(k, SLOTS)
        for p in range(3):
            cols, (b1, b2, b3), (_, _, to) = geometry(p, k)
            place = mine_at(k, q1 * b1 + q2 * b2 + q3 * b3, q3)
            kept[place, cols] = (acc[a, at(q2 * b2 + q3 * b3, q3), cols]
                                 + kept[spare_at(k, q1 + q2, q3), cols].astype(F32)).astype(BF)
            send(kept.at[place, cols], kept.at[place, cols], AG3, k, to)
        pl.semaphore_signal(credit, inc=1, device_id={"tp": partner}, device_id_type=MESH)

    def gather(k, got, stage, span, which):
        await_bytes(got, k, rsem)
        for p in range(3):
            cols, (b1, b2, _), tos = geometry(p, k)
            place = mine_at(k, q1 * b1 + q2 * b2 if which == 1 else q1 * b1, span)
            send(kept.at[place, cols], kept.at[place, cols], stage, k, tos[which])

    def stage5(k):
        gather(k, AG3, AG2, q2, 1)

    def stage6(k):
        gather(k, AG2, AG1, q1, 0)

    def stage7(k):
        await_bytes(AG1, k, rsem)
        pl.semaphore_wait(credit, 1)
        place = mine_at(k, 0, HALF)
        send(kept.at[place], kept.at[place], DG, k, partner)

    stages = (stage0, stage1, stage2, stage3, stage4, stage5, stage6, stage7)

    def run(base, n, per, i, j):
        for stage in PRIO:
            turns = [(k, (p - base) // per) for k, p in enumerate(POINTS[stage - 1])
                     if base <= p < base + n * per and (p - base) % per == j]
            if turns:
                k = sum(jnp.where(i == t, k, 0) for k, t in turns)
                now = functools.reduce(jnp.logical_or, [i == t for _, t in turns])

                @pl.when(now)
                def _():
                    stages[stage](k)

    def slot1(bufs, s):
        dyb, gb, ub = bufs
        q = lax.rem(s, 2)

        @pl.when(s + 1 < n_chunks)
        def _():
            for c in load_chunk(s + 1, 1 - q, *bufs):
                c.start()

        @pl.when(s == 0)
        def _():
            download.wait()

        for c in load_chunk(s, q, *bufs):
            c.wait()

        base = pl.multiple_of(s * CHUNK, CHUNK)
        dh = lax.dot_general(dyb[q], kept[down], NT, preferred_element_type=F32)
        g, u = gb[q].astype(F32), ub[q].astype(F32)
        g2 = g * g
        t = jnp.tanh((C0 * g) * (1.0 + C1 * g2))
        cdf = 0.5 + 0.5 * t
        gelu = g * cdf
        slope = cdf + g * (cdf * (1.0 - t)) * (C0 + (3.0 * C0 * C1) * g2)
        hidt[:, pl.ds(base, CHUNK)] = (gelu * u).astype(BF).T
        dgu[pl.ds(base, CHUNK), 0:ff] = (dh * u * slope).astype(BF)
        dgu[pl.ds(base, CHUNK), ff:2 * ff] = (dh * gelu).astype(BF)

        @pl.when(s == 0)
        def _():
            for pair in wloads:
                for c in pair:
                    c.wait()

        run(0, n_chunks, 2, s, 0)
        theirs = pl.ds(pl.multiple_of(base + HALF * (1 - core), HALF), HALF)
        mine = pl.ds(pl.multiple_of(base + HALF * core, HALF), HALF)
        lhs = jnp.concatenate([dgu[theirs], dgu[mine]], axis=0)
        for n in range(2):
            cols = slice(n * (dim // 2), (n + 1) * (dim // 2))
            rhs = jnp.concatenate([weight(w, cols.start, cols.stop) for w in range(2)], axis=1)
            term = lax.dot_general(lhs, rhs, NT, preferred_element_type=F32)
            pbuf[:, cols] = term[:HALF].astype(BF)
            own[:, cols] = term[HALF:]
        stage0(s)
        run(0, n_chunks, 2, s, 1)

    def phase1(*bufs):
        for c in load_chunk(0, 0, *bufs):
            c.start()
        for pair in wloads:
            for c in pair:
                c.start()
        pl.semaphore_wait(barrier, 4)

        def body(s, _):
            slot1(bufs, s)
            return ()

        lax.fori_loop(0, n_chunks, body, ())

    pl.run_scoped(phase1, pltpu.VMEM((2, CHUNK, dim), BF), pltpu.VMEM((2, CHUNK, ff), BF), pltpu.VMEM((2, CHUNK, ff), BF))

    base2 = n_chunks * 2

    def slot2(bufs, t):
        q = lax.rem(t, 3)

        @pl.when(t + 2 < n_tiles)
        def _():
            for c in load_col(t + 2, lax.rem(t + 2, 3), *bufs):
                c.start()

        xcol, dycol = bufs
        loads = load_col(t, q, *bufs)
        r = pl.ds(pl.multiple_of(t * TILE, TILE), TILE)
        loads[0].wait()
        loads[1].wait()
        dw = lax.dot_general(xcol[q], dgu[...], TN, preferred_element_type=F32)
        dw = dw.astype(BF)
        for i in range(TILE // 128):
            row = t * TILE + i * 128
            lanes = pl.ds(pl.multiple_of((row // ff) * ff, 128), ff)
            for w in range(2):
                place = pl.ds(pl.multiple_of(starts[w] + row % ff, 128), 128)
                kept[place, lanes] = dw[i * 128:(i + 1) * 128, w * ff:(w + 1) * ff]
        kept[down, r] = lax.dot_general(hidt[...], dycol[q], NN, preferred_element_type=F32).astype(BF)
        run(base2, n_tiles, 1, t, 0)

    def phase2(*bufs):
        for t in range(2):
            for c in load_col(t, t, *bufs):
                c.start()

        def body(t, _):
            slot2(bufs, t)
            return ()

        lax.fori_loop(0, n_tiles, body, ())

    pl.run_scoped(phase2, pltpu.VMEM((3, rows, TILE), BF), pltpu.VMEM((3, rows, TILE), BF))

    rest = sorted((p, PRIO.index(stage), stage, k) for stage in range(1, 8) for k, p in enumerate(POINTS[stage - 1])
                  if p >= base2 + n_tiles)
    for _, _, stage, k in rest:
        stages[stage](k)

    def finish(k, _):
        await_bytes(DG, k, rsem)
        for stage in (AG3, AG2, AG1, DG):
            await_bytes(stage, k, ssem)

        @pl.when(k >= n_chunks - SLOTS)
        def _():
            for stage in (RS1, RS2, RS3):
                await_bytes(stage, k, ssem)

        return ()

    lax.fori_loop(0, n_chunks, finish, ())


def writer(kept, dx, dwg, dwu, dwd, sem):
    rows, (dim, ff) = dx.shape[0], dwg.shape
    pairs = [(kept.at[i * 256:(i + 1) * 256], dx.at[i * 256:(i + 1) * 256]) for i in range(rows // 256)]
    pairs += [(kept.at[rows + i * 128:rows + (i + 1) * 128], dwd.at[i * 128:(i + 1) * 128]) for i in range(ff // 128)]
    for w, out in enumerate((dwg, dwu)):
        start = rows + (1 + w) * ff
        pairs += [(kept.at[start:start + ff, b * ff:(b + 1) * ff], out.at[b * ff:(b + 1) * ff]) for b in range(dim // ff)]
    copies = [pltpu.make_async_copy(a, b, sem.at[i]) for i, (a, b) in enumerate(pairs)]
    for c in copies:
        c.start()
    for c in copies:
        c.wait()


def backward(x, dy, gate, up, w_gate, w_up, w_down):
    rows, dim = x.shape
    ff = gate.shape[1]
    n_chunks, n_blocks = rows // CHUNK, dim // ff
    hbm, inside = pl.BlockSpec(memory_space=pl.ANY), pl.BlockSpec(memory_space=pltpu.VMEM)
    vmem, dma = pltpu.VMEM, pltpu.SemaphoreType.DMA
    kept = pl.pallas_call(
        kernel,
        out_shape=vmem((rows + 3 * ff, dim), BF),
        in_specs=[hbm] * 7,
        out_specs=inside,
        scratch_shapes=[
            vmem((rows, 2 * ff), BF), vmem((ff, rows), BF), vmem((HALF, dim), BF), vmem((HALF, dim), F32),
            vmem((SLOTS, HALF // 8 * 7, dim), BF), vmem((SLOTS, HALF // 2, dim), F32),
            dma((2 * n_blocks + 1,)), dma((3, 2)), dma((2, 3)), pltpu.SemaphoreType.REGULAR,
            dma((8, n_chunks)), dma((8, n_chunks)),
        ],
        compiler_params=pltpu.CompilerParams(collective_id=0, has_side_effects=True, vmem_limit_bytes=VMEM_LIMIT),
        name="mlp_backward",
    )(x, dy, gate, up, w_gate, w_up, w_down)
    return pl.pallas_call(
        writer,
        out_shape=tuple(jax.ShapeDtypeStruct(g, BF) for g in ((rows, dim), (dim, ff), (dim, ff), (ff, dim))),
        in_specs=[inside],
        out_specs=(hbm,) * 4,
        scratch_shapes=[dma((2 * n_blocks + rows // 256 + ff // 128,))],
        compiler_params=pltpu.CompilerParams(vmem_limit_bytes=WRITER_LIMIT),
        name="writer",
    )(kept)


def solution(mesh):
    tokens, columns, rows = P("dp", None), P(None, "tp"), P("tp", None)
    return jax.shard_map(
        backward,
        mesh=mesh,
        in_specs=(tokens, tokens, P("dp", "tp"), P("dp", "tp"), columns, columns, rows),
        out_specs=(tokens, P("dp", "tp"), P("dp", "tp"), P(("dp", "tp"), None)),
        check_vma=False,
    )
```

```python
import functools

import jax
import jax.numpy as jnp
from jax import lax
from jax.experimental import pallas as pl
from jax.experimental.pallas import tpu as pltpu
from jax.sharding import PartitionSpec as P

MESH = pl.DeviceIdType.MESH
BF, F32 = jnp.bfloat16, jnp.float32
CHUNK = 256
HALF = CHUNK // 2
SLOTS = 4
VMEM_LIMIT, WRITER_LIMIT = 32_000_000, 1_000_000
TILE = 256
C0 = 0.7978845608028654
C1 = 0.044715
STRIDES = (8, 4, 2)
NT = (((1,), (1,)), ((), ()))
TN = (((0,), (0,)), ((), ()))
NN = (((1,), (0,)), ((), ()))
D, RS1, RS2, RS3, AG3, AG2, AG1, DG = range(8)
ROWS_OF = (HALF, HALF // 2, HALF // 4, HALF // 8, HALF // 8, HALF // 4, HALF // 2, HALF)

POINTS = (
    (2, 4, 6, 8, 10, 12, 14, 16),
    (4, 7, 8, 11, 12, 15, 18, 19),
    (6, 9, 10, 14, 17, 18, 20, 21),
    (7, 11, 12, 16, 20, 21, 22, 23),
    (9, 13, 14, 18, 22, 23, 24, 25),
    (11, 20, 22, 25, 26, 27, 28, 30),
    (14, 23, 25, 28, 29, 31, 32, 33),
)
PRIO = (4, 3, 2, 5, 1, 7, 6)


def kernel(x, dy, gate, up, w_gate, w_up, w_down, kept, dgu, hidt, pbuf, own, staged, acc,
           wsem, insem, colsem, credit, ssem, rsem):
    rows, dim = x.shape
    ff = gate.shape[1]
    n_chunks = rows // CHUNK
    n_tiles = dim // TILE
    n_blocks = dim // ff
    down = slice(rows, rows + ff)
    starts = (rows + ff, rows + 2 * ff)

    units = dim // 128
    w2 = units // 3
    w0 = units - 2 * w2
    parts = ((0, w0 * 128), (w0 * 128, w2 * 128), ((w0 + w2) * 128, w2 * 128))

    me = lax.axis_index("tp")
    core = me % 2
    bits = tuple((me // s) % 2 for s in STRIDES)
    near = tuple(me + s - 2 * s * b for s, b in zip(STRIDES, bits))
    partner = me + 1 - 2 * core

    def load_chunk(k, slot, dyb, gb, ub):
        r = pl.ds(pl.multiple_of(k * CHUNK, CHUNK), CHUNK)
        return (pltpu.make_async_copy(dy.at[r], dyb.at[slot], insem.at[0, slot]),
                pltpu.make_async_copy(gate.at[r], gb.at[slot], insem.at[1, slot]),
                pltpu.make_async_copy(up.at[r], ub.at[slot], insem.at[2, slot]))

    def load_col(t, q, xcol, dycol):
        c = pl.ds(pl.multiple_of(t * TILE, TILE), TILE)
        return (pltpu.make_async_copy(x.at[:, c], xcol.at[q], colsem.at[0, q]),
                pltpu.make_async_copy(dy.at[:, c], dycol.at[q], colsem.at[1, q]))

    def block(w, b):
        return slice(starts[w], starts[w] + ff), slice(b * ff, (b + 1) * ff)

    def weight(w, lo, hi):
        pieces = []
        while lo < hi:
            b = lo // ff
            end = min(hi, (b + 1) * ff)
            pieces.append(kept[starts[w] + lo - b * ff:starts[w] + end - b * ff, b * ff:(b + 1) * ff])
            lo = end
        return jnp.concatenate(pieces, axis=0)

    download = pltpu.make_async_copy(w_down, kept.at[down], wsem.at[2 * n_blocks])
    wloads = tuple(tuple(pltpu.make_async_copy(src.at[b * ff:(b + 1) * ff], kept.at[block(w, b)], wsem.at[2 * b + w])
                         for w, src in enumerate((w_gate, w_up))) for b in range(n_blocks))
    download.start()

    barrier = pltpu.get_barrier_semaphore()
    for other in (*near, partner):
        pl.semaphore_signal(barrier, inc=1, device_id={"tp": other}, device_id_type=MESH)

    def send(src, dst, stage, k, to):
        pltpu.make_async_remote_copy(src_ref=src, dst_ref=dst, send_sem=ssem.at[stage, k], recv_sem=rsem.at[stage, k],
                                     device_id={"tp": to}, device_id_type=MESH).start()

    def await_bytes(stage, k, sems):
        ref = kept.at[0:ROWS_OF[stage]]
        pltpu.make_async_copy(ref, ref, sems.at[stage, k]).wait()

    def pick(values, i):
        return jnp.where(i == 0, values[0], jnp.where(i == 1, values[1], values[2]))

    def geometry(p, k):
        c0, cw = parts[p]
        dims = [lax.rem(p + k + i, 3) for i in range(3)]
        return slice(c0, c0 + cw), [pick(bits, d) for d in dims], [pick(near, d) for d in dims]

    def at(o, n):
        return pl.ds(pl.multiple_of(o, HALF // 8), n)

    def mine_at(k, o, n):
        return at(k * CHUNK + HALF * core + o, n)

    def spare_at(k, o, n):
        return at(k * CHUNK + HALF * (1 - core) + o, n)

    def stage0(k):
        send(pbuf, kept.at[spare_at(k, 0, HALF)], D, k, partner)

    q1, q2, q3 = HALF // 2, HALF // 4, HALF // 8

    def stage1(k):
        await_bytes(D, k, ssem)
        await_bytes(D, k, rsem)

        @pl.when(k >= SLOTS)
        def _():
            for stage in (RS1, RS2, RS3):
                await_bytes(stage, k - SLOTS, ssem)

        a = lax.rem(k, SLOTS)
        for p in range(3):
            cols, (b1, _, _), (to, _, _) = geometry(p, k)
            out, keep = q1 * (1 - b1), q1 * b1
            staged[a, 0:q1, cols] = (own[at(out, q1), cols] + kept[mine_at(k, out, q1), cols].astype(F32)).astype(BF)
            send(staged.at[a, 0:q1, cols], kept.at[spare_at(k, 0, q1), cols], RS1, k, to)
            acc[a, :, cols] = own[at(keep, q1), cols] + kept[mine_at(k, keep, q1), cols].astype(F32)

    def stage2(k):
        await_bytes(RS1, k, rsem)
        a = lax.rem(k, SLOTS)
        for p in range(3):
            cols, (_, b2, _), (_, to, _) = geometry(p, k)
            out, keep = q2 * (1 - b2), q2 * b2
            stage = slice(q1, q1 + q2)
            staged[a, stage, cols] = (acc[a, at(out, q2), cols] + kept[spare_at(k, out, q2), cols].astype(F32)).astype(BF)
            send(staged.at[a, stage, cols], kept.at[spare_at(k, q1, q2), cols], RS2, k, to)
            acc[a, at(keep, q2), cols] = acc[a, at(keep, q2), cols] + kept[spare_at(k, keep, q2), cols].astype(F32)

    def stage3(k):
        await_bytes(RS2, k, rsem)
        a = lax.rem(k, SLOTS)
        for p in range(3):
            cols, (_, b2, b3), (_, _, to) = geometry(p, k)
            out, keep = q3 * (1 - b3), q3 * b3
            stage = slice(q1 + q2, q1 + q2 + q3)
            staged[a, stage, cols] = (acc[a, at(q2 * b2 + out, q3), cols]
                                      + kept[spare_at(k, q1 + out, q3), cols].astype(F32)).astype(BF)
            send(staged.at[a, stage, cols], kept.at[spare_at(k, q1 + q2, q3), cols], RS3, k, to)
            place = at(q2 * b2 + keep, q3)
            acc[a, place, cols] = acc[a, place, cols] + kept[spare_at(k, q1 + keep, q3), cols].astype(F32)

    def stage4(k):
        await_bytes(RS3, k, rsem)
        a = lax.rem(k, SLOTS)
        for p in range(3):
            cols, (b1, b2, b3), (_, _, to) = geometry(p, k)
            place = mine_at(k, q1 * b1 + q2 * b2 + q3 * b3, q3)
            kept[place, cols] = (acc[a, at(q2 * b2 + q3 * b3, q3), cols]
                                 + kept[spare_at(k, q1 + q2, q3), cols].astype(F32)).astype(BF)
            send(kept.at[place, cols], kept.at[place, cols], AG3, k, to)
        pl.semaphore_signal(credit, inc=1, device_id={"tp": partner}, device_id_type=MESH)

    def gather(k, got, stage, span, which):
        await_bytes(got, k, rsem)
        for p in range(3):
            cols, (b1, b2, _), tos = geometry(p, k)
            place = mine_at(k, q1 * b1 + q2 * b2 if which == 1 else q1 * b1, span)
            send(kept.at[place, cols], kept.at[place, cols], stage, k, tos[which])

    def stage5(k):
        gather(k, AG3, AG2, q2, 1)

    def pass_on(k, ours):
        for p in range(3):
            cols, (b1, _, _), _ = geometry(p, k)
            place = mine_at(k, q1 * b1 if ours else q1 * (1 - b1), q1)
            send(kept.at[place, cols], kept.at[place, cols], DG, k, partner)

    def stage6(k):
        gather(k, AG2, AG1, q1, 0)
        pl.semaphore_wait(credit, 1)
        pass_on(k, True)

    def stage7(k):
        await_bytes(AG1, k, rsem)
        pass_on(k, False)

    stages = (stage0, stage1, stage2, stage3, stage4, stage5, stage6, stage7)

    def run(base, n, per, i, j):
        for stage in PRIO:
            turns = [(k, (p - base) // per) for k, p in enumerate(POINTS[stage - 1])
                     if base <= p < base + n * per and (p - base) % per == j]
            if turns:
                k = sum(jnp.where(i == t, k, 0) for k, t in turns)
                now = functools.reduce(jnp.logical_or, [i == t for _, t in turns])

                @pl.when(now)
                def _():
                    stages[stage](k)

    def slot1(bufs, s):
        dyb, gb, ub = bufs
        q = lax.rem(s, 2)

        @pl.when(s + 1 < n_chunks)
        def _():
            for c in load_chunk(s + 1, 1 - q, *bufs):
                c.start()

        @pl.when(s == 0)
        def _():
            download.wait()

        for c in load_chunk(s, q, *bufs):
            c.wait()

        base = pl.multiple_of(s * CHUNK, CHUNK)
        dh = lax.dot_general(dyb[q], kept[down], NT, preferred_element_type=F32)
        g, u = gb[q].astype(F32), ub[q].astype(F32)
        g2 = g * g
        t = jnp.tanh((C0 * g) * (1.0 + C1 * g2))
        cdf = 0.5 + 0.5 * t
        gelu = g * cdf
        slope = cdf + g * (cdf * (1.0 - t)) * (C0 + (3.0 * C0 * C1) * g2)
        hidt[:, pl.ds(base, CHUNK)] = (gelu * u).astype(BF).T
        dgu[pl.ds(base, CHUNK), 0:ff] = (dh * u * slope).astype(BF)
        dgu[pl.ds(base, CHUNK), ff:2 * ff] = (dh * gelu).astype(BF)

        @pl.when(s == 0)
        def _():
            for pair in wloads:
                for c in pair:
                    c.wait()

        run(0, n_chunks, 2, s, 0)
        theirs = pl.ds(pl.multiple_of(base + HALF * (1 - core), HALF), HALF)
        mine = pl.ds(pl.multiple_of(base + HALF * core, HALF), HALF)
        lhs = jnp.concatenate([dgu[theirs], dgu[mine]], axis=0)
        for n in range(2):
            cols = slice(n * (dim // 2), (n + 1) * (dim // 2))
            rhs = jnp.concatenate([weight(w, cols.start, cols.stop) for w in range(2)], axis=1)
            term = lax.dot_general(lhs, rhs, NT, preferred_element_type=F32)
            pbuf[:, cols] = term[:HALF].astype(BF)
            own[:, cols] = term[HALF:]
        stage0(s)
        run(0, n_chunks, 2, s, 1)

    def phase1(*bufs):
        for c in load_chunk(0, 0, *bufs):
            c.start()
        for pair in wloads:
            for c in pair:
                c.start()
        pl.semaphore_wait(barrier, 4)

        def body(s, _):
            slot1(bufs, s)
            return ()

        lax.fori_loop(0, n_chunks, body, ())

    pl.run_scoped(phase1, pltpu.VMEM((2, CHUNK, dim), BF), pltpu.VMEM((2, CHUNK, ff), BF), pltpu.VMEM((2, CHUNK, ff), BF))

    base2 = n_chunks * 2

    def slot2(bufs, t):
        q = lax.rem(t, 3)

        @pl.when(t + 2 < n_tiles)
        def _():
            for c in load_col(t + 2, lax.rem(t + 2, 3), *bufs):
                c.start()

        xcol, dycol = bufs
        loads = load_col(t, q, *bufs)
        r = pl.ds(pl.multiple_of(t * TILE, TILE), TILE)
        loads[0].wait()
        loads[1].wait()
        dw = lax.dot_general(xcol[q], dgu[...], TN, preferred_element_type=F32)
        dw = dw.astype(BF)
        for i in range(TILE // 128):
            row = t * TILE + i * 128
            lanes = pl.ds(pl.multiple_of((row // ff) * ff, 128), ff)
            for w in range(2):
                place = pl.ds(pl.multiple_of(starts[w] + row % ff, 128), 128)
                kept[place, lanes] = dw[i * 128:(i + 1) * 128, w * ff:(w + 1) * ff]
        kept[down, r] = lax.dot_general(hidt[...], dycol[q], NN, preferred_element_type=F32).astype(BF)
        run(base2, n_tiles, 1, t, 0)

    def phase2(*bufs):
        for t in range(2):
            for c in load_col(t, t, *bufs):
                c.start()

        def body(t, _):
            slot2(bufs, t)
            return ()

        lax.fori_loop(0, n_tiles, body, ())

    pl.run_scoped(phase2, pltpu.VMEM((3, rows, TILE), BF), pltpu.VMEM((3, rows, TILE), BF))

    rest = sorted((p, PRIO.index(stage), stage, k) for stage in range(1, 8) for k, p in enumerate(POINTS[stage - 1])
                  if p >= base2 + n_tiles)
    for _, _, stage, k in rest:
        stages[stage](k)

    def finish(k, _):
        await_bytes(DG, k, rsem)
        for stage in (AG3, AG2, AG1, DG):
            await_bytes(stage, k, ssem)

        @pl.when(k >= n_chunks - SLOTS)
        def _():
            for stage in (RS1, RS2, RS3):
                await_bytes(stage, k, ssem)

        return ()

    lax.fori_loop(0, n_chunks, finish, ())


def writer(kept, dx, dwg, dwu, dwd, sem):
    rows, (dim, ff) = dx.shape[0], dwg.shape
    pairs = [(kept.at[i * 256:(i + 1) * 256], dx.at[i * 256:(i + 1) * 256]) for i in range(rows // 256)]
    pairs += [(kept.at[rows + i * 128:rows + (i + 1) * 128], dwd.at[i * 128:(i + 1) * 128]) for i in range(ff // 128)]
    for w, out in enumerate((dwg, dwu)):
        start = rows + (1 + w) * ff
        pairs += [(kept.at[start:start + ff, b * ff:(b + 1) * ff], out.at[b * ff:(b + 1) * ff]) for b in range(dim // ff)]
    copies = [pltpu.make_async_copy(a, b, sem.at[i]) for i, (a, b) in enumerate(pairs)]
    for c in copies:
        c.start()
    for c in copies:
        c.wait()


def backward(x, dy, gate, up, w_gate, w_up, w_down):
    rows, dim = x.shape
    ff = gate.shape[1]
    n_chunks, n_blocks = rows // CHUNK, dim // ff
    hbm, inside = pl.BlockSpec(memory_space=pl.ANY), pl.BlockSpec(memory_space=pltpu.VMEM)
    vmem, dma = pltpu.VMEM, pltpu.SemaphoreType.DMA
    kept = pl.pallas_call(
        kernel,
        out_shape=vmem((rows + 3 * ff, dim), BF),
        in_specs=[hbm] * 7,
        out_specs=inside,
        scratch_shapes=[
            vmem((rows, 2 * ff), BF), vmem((ff, rows), BF), vmem((HALF, dim), BF), vmem((HALF, dim), F32),
            vmem((SLOTS, HALF // 8 * 7, dim), BF), vmem((SLOTS, HALF // 2, dim), F32),
            dma((2 * n_blocks + 1,)), dma((3, 2)), dma((2, 3)), pltpu.SemaphoreType.REGULAR,
            dma((8, n_chunks)), dma((8, n_chunks)),
        ],
        compiler_params=pltpu.CompilerParams(collective_id=0, has_side_effects=True, vmem_limit_bytes=VMEM_LIMIT),
        name="mlp_backward",
    )(x, dy, gate, up, w_gate, w_up, w_down)
    return pl.pallas_call(
        writer,
        out_shape=tuple(jax.ShapeDtypeStruct(g, BF) for g in ((rows, dim), (dim, ff), (dim, ff), (ff, dim))),
        in_specs=[inside],
        out_specs=(hbm,) * 4,
        scratch_shapes=[dma((2 * n_blocks + rows // 256 + ff // 128,))],
        compiler_params=pltpu.CompilerParams(vmem_limit_bytes=WRITER_LIMIT),
        name="writer",
    )(kept)


def solution(mesh):
    tokens, columns, rows = P("dp", None), P(None, "tp"), P("tp", None)
    return jax.shard_map(
        backward,
        mesh=mesh,
        in_specs=(tokens, tokens, P("dp", "tp"), P("dp", "tp"), columns, columns, rows),
        out_specs=(tokens, P("dp", "tp"), P("dp", "tp"), P(("dp", "tp"), None)),
        check_vma=False,
    )
```

```python
import functools

import jax
import jax.numpy as jnp
from jax import lax
from jax.experimental import pallas as pl
from jax.experimental.pallas import tpu as pltpu
from jax.sharding import PartitionSpec as P

MESH = pl.DeviceIdType.MESH
BF, F32 = jnp.bfloat16, jnp.float32
CHUNK = 256
HALF = CHUNK // 2
SLOTS = 4
VMEM_LIMIT, WRITER_LIMIT = 32_000_000, 1_000_000
TILE = 256
C0 = 0.7978845608028654
C1 = 0.044715
STRIDES = (8, 4, 2)
NT = (((1,), (1,)), ((), ()))
TN = (((0,), (0,)), ((), ()))
NN = (((1,), (0,)), ((), ()))
D, RS1, RS2, RS3, AG3, AG2, AG1, DG = range(8)
ROWS_OF = (HALF, HALF // 2, HALF // 4, HALF // 8, HALF // 8, HALF // 4, HALF // 2, HALF)

POINTS = (
    (2, 4, 6, 8, 10, 12, 14, 16),
    (4, 7, 8, 11, 12, 15, 18, 19),
    (6, 9, 10, 14, 17, 18, 20, 21),
    (7, 11, 12, 16, 20, 21, 22, 23),
    (9, 13, 14, 18, 22, 23, 24, 25),
    (11, 20, 22, 25, 26, 27, 28, 30),
    (14, 23, 25, 28, 29, 31, 32, 33),
)
PRIO = (4, 3, 2, 5, 1, 7, 6)


def kernel(x, dy, gate, up, w_gate, w_up, w_down, kept, dgu, hidt, pbuf, own, staged, acc,
           wsem, insem, colsem, credit, ssem, rsem):
    rows, dim = x.shape
    ff = gate.shape[1]
    n_chunks = rows // CHUNK
    n_tiles = dim // TILE
    n_blocks = dim // ff
    down = slice(rows, rows + ff)
    starts = (rows + ff, rows + 2 * ff)

    units = dim // 128
    w2 = units // 3
    w0 = units - 2 * w2
    parts = ((0, w0 * 128), (w0 * 128, w2 * 128), ((w0 + w2) * 128, w2 * 128))

    me = lax.axis_index("tp")
    core = me % 2
    bits = tuple((me // s) % 2 for s in STRIDES)
    near = tuple(me + s - 2 * s * b for s, b in zip(STRIDES, bits))
    partner = me + 1 - 2 * core

    def load_chunk(k, slot, dyb, gb, ub):
        r = pl.ds(pl.multiple_of(k * CHUNK, CHUNK), CHUNK)
        return (pltpu.make_async_copy(dy.at[r], dyb.at[slot], insem.at[0, slot]),
                pltpu.make_async_copy(gate.at[r], gb.at[slot], insem.at[1, slot]),
                pltpu.make_async_copy(up.at[r], ub.at[slot], insem.at[2, slot]))

    def load_col(t, q, xcol, dycol):
        c = pl.ds(pl.multiple_of(t * TILE, TILE), TILE)
        return (pltpu.make_async_copy(x.at[:, c], xcol.at[q], colsem.at[0, q]),
                pltpu.make_async_copy(dy.at[:, c], dycol.at[q], colsem.at[1, q]))

    def block(w, b):
        return slice(starts[w], starts[w] + ff), slice(b * ff, (b + 1) * ff)

    def weight(w, lo, hi):
        pieces = []
        while lo < hi:
            b = lo // ff
            end = min(hi, (b + 1) * ff)
            pieces.append(kept[starts[w] + lo - b * ff:starts[w] + end - b * ff, b * ff:(b + 1) * ff])
            lo = end
        return jnp.concatenate(pieces, axis=0)

    download = pltpu.make_async_copy(w_down, kept.at[down], wsem.at[2 * n_blocks])
    wloads = tuple(tuple(pltpu.make_async_copy(src.at[b * ff:(b + 1) * ff], kept.at[block(w, b)], wsem.at[2 * b + w])
                         for w, src in enumerate((w_gate, w_up))) for b in range(n_blocks))
    download.start()

    barrier = pltpu.get_barrier_semaphore()
    for other in (*near, partner):
        pl.semaphore_signal(barrier, inc=1, device_id={"tp": other}, device_id_type=MESH)

    def send(src, dst, stage, k, to):
        pltpu.make_async_remote_copy(src_ref=src, dst_ref=dst, send_sem=ssem.at[stage, k], recv_sem=rsem.at[stage, k],
                                     device_id={"tp": to}, device_id_type=MESH).start()

    def await_bytes(stage, k, sems):
        ref = kept.at[0:ROWS_OF[stage]]
        pltpu.make_async_copy(ref, ref, sems.at[stage, k]).wait()

    def pick(values, i):
        return jnp.where(i == 0, values[0], jnp.where(i == 1, values[1], values[2]))

    def geometry(p, k):
        c0, cw = parts[p]
        dims = [lax.rem(p + k + i, 3) for i in range(3)]
        return slice(c0, c0 + cw), [pick(bits, d) for d in dims], [pick(near, d) for d in dims]

    def at(o, n):
        return pl.ds(pl.multiple_of(o, HALF // 8), n)

    def mine_at(k, o, n):
        return at(k * CHUNK + HALF * core + o, n)

    def spare_at(k, o, n):
        return at(k * CHUNK + HALF * (1 - core) + o, n)

    def stage0(k):
        send(pbuf, kept.at[spare_at(k, 0, HALF)], D, k, partner)

    q1, q2, q3 = HALF // 2, HALF // 4, HALF // 8

    def stage1(k):
        await_bytes(D, k, ssem)
        await_bytes(D, k, rsem)

        @pl.when(k >= SLOTS)
        def _():
            for stage in (RS1, RS2, RS3):
                await_bytes(stage, k - SLOTS, ssem)

        a = lax.rem(k, SLOTS)
        for p in range(3):
            cols, (b1, _, _), (to, _, _) = geometry(p, k)
            out = q1 * (1 - b1)
            staged[a, 0:q1, cols] = (own[at(out, q1), cols] + kept[mine_at(k, out, q1), cols].astype(F32)).astype(BF)
            send(staged.at[a, 0:q1, cols], kept.at[spare_at(k, 0, q1), cols], RS1, k, to)

        for p in range(3):
            cols, (b1, _, _), _ = geometry(p, k)
            keep = q1 * b1
            acc[a, :, cols] = own[at(keep, q1), cols] + kept[mine_at(k, keep, q1), cols].astype(F32)

    def stage2(k):
        await_bytes(RS1, k, rsem)
        a = lax.rem(k, SLOTS)
        for p in range(3):
            cols, (_, b2, _), (_, to, _) = geometry(p, k)
            out = q2 * (1 - b2)
            stage = slice(q1, q1 + q2)
            staged[a, stage, cols] = (acc[a, at(out, q2), cols] + kept[spare_at(k, out, q2), cols].astype(F32)).astype(BF)
            send(staged.at[a, stage, cols], kept.at[spare_at(k, q1, q2), cols], RS2, k, to)

        for p in range(3):
            cols, (_, b2, _), _ = geometry(p, k)
            keep = q2 * b2
            acc[a, at(keep, q2), cols] = acc[a, at(keep, q2), cols] + kept[spare_at(k, keep, q2), cols].astype(F32)

    def stage3(k):
        await_bytes(RS2, k, rsem)
        a = lax.rem(k, SLOTS)
        for p in range(3):
            cols, (_, b2, b3), (_, _, to) = geometry(p, k)
            out = q3 * (1 - b3)
            stage = slice(q1 + q2, q1 + q2 + q3)
            staged[a, stage, cols] = (acc[a, at(q2 * b2 + out, q3), cols]
                                      + kept[spare_at(k, q1 + out, q3), cols].astype(F32)).astype(BF)
            send(staged.at[a, stage, cols], kept.at[spare_at(k, q1 + q2, q3), cols], RS3, k, to)

        for p in range(3):
            cols, (_, b2, b3), _ = geometry(p, k)
            keep = q3 * b3
            place = at(q2 * b2 + keep, q3)
            acc[a, place, cols] = acc[a, place, cols] + kept[spare_at(k, q1 + keep, q3), cols].astype(F32)

    def stage4(k):
        await_bytes(RS3, k, rsem)
        a = lax.rem(k, SLOTS)
        for p in range(3):
            cols, (b1, b2, b3), (_, _, to) = geometry(p, k)
            place = mine_at(k, q1 * b1 + q2 * b2 + q3 * b3, q3)
            kept[place, cols] = (acc[a, at(q2 * b2 + q3 * b3, q3), cols]
                                 + kept[spare_at(k, q1 + q2, q3), cols].astype(F32)).astype(BF)
            send(kept.at[place, cols], kept.at[place, cols], AG3, k, to)
        pl.semaphore_signal(credit, inc=1, device_id={"tp": partner}, device_id_type=MESH)

    def gather(k, got, stage, span, which):
        await_bytes(got, k, rsem)
        for p in range(3):
            cols, (b1, b2, _), tos = geometry(p, k)
            place = mine_at(k, q1 * b1 + q2 * b2 if which == 1 else q1 * b1, span)
            send(kept.at[place, cols], kept.at[place, cols], stage, k, tos[which])

    def stage5(k):
        gather(k, AG3, AG2, q2, 1)

    def pass_on(k, ours):
        for p in range(3):
            cols, (b1, _, _), _ = geometry(p, k)
            place = mine_at(k, q1 * b1 if ours else q1 * (1 - b1), q1)
            send(kept.at[place, cols], kept.at[place, cols], DG, k, partner)

    def stage6(k):
        gather(k, AG2, AG1, q1, 0)
        pl.semaphore_wait(credit, 1)
        pass_on(k, True)

    def stage7(k):
        await_bytes(AG1, k, rsem)
        pass_on(k, False)

    stages = (stage0, stage1, stage2, stage3, stage4, stage5, stage6, stage7)

    def run(base, n, per, i, j):
        for stage in PRIO:
            turns = [(k, (p - base) // per) for k, p in enumerate(POINTS[stage - 1])
                     if base <= p < base + n * per and (p - base) % per == j]
            if turns:
                k = sum(jnp.where(i == t, k, 0) for k, t in turns)
                now = functools.reduce(jnp.logical_or, [i == t for _, t in turns])

                @pl.when(now)
                def _():
                    stages[stage](k)

    def slot1(bufs, s):
        dyb, gb, ub = bufs
        q = lax.rem(s, 2)

        @pl.when(s + 1 < n_chunks)
        def _():
            for c in load_chunk(s + 1, 1 - q, *bufs):
                c.start()

        @pl.when(s == 0)
        def _():
            download.wait()

        for c in load_chunk(s, q, *bufs):
            c.wait()

        base = pl.multiple_of(s * CHUNK, CHUNK)
        dh = lax.dot_general(dyb[q], kept[down], NT, preferred_element_type=F32)
        g, u = gb[q].astype(F32), ub[q].astype(F32)
        g2 = g * g
        t = jnp.tanh((C0 * g) * (1.0 + C1 * g2))
        cdf = 0.5 + 0.5 * t
        gelu = g * cdf
        slope = cdf + g * (cdf * (1.0 - t)) * (C0 + (3.0 * C0 * C1) * g2)
        hidt[:, pl.ds(base, CHUNK)] = (gelu * u).astype(BF).T
        dgu[pl.ds(base, CHUNK), 0:ff] = (dh * u * slope).astype(BF)
        dgu[pl.ds(base, CHUNK), ff:2 * ff] = (dh * gelu).astype(BF)

        @pl.when(s == 0)
        def _():
            for pair in wloads:
                for c in pair:
                    c.wait()

        run(0, n_chunks, 2, s, 0)
        theirs = pl.ds(pl.multiple_of(base + HALF * (1 - core), HALF), HALF)
        mine = pl.ds(pl.multiple_of(base + HALF * core, HALF), HALF)
        lhs = jnp.concatenate([dgu[theirs], dgu[mine]], axis=0)
        for cols in (slice(0, dim),):
            rhs = jnp.concatenate([weight(w, cols.start, cols.stop) for w in range(2)], axis=1)
            term = lax.dot_general(lhs, rhs, NT, preferred_element_type=F32)
            pbuf[:, cols] = term[:HALF].astype(BF)
            own[:, cols] = term[HALF:]
        stage0(s)
        run(0, n_chunks, 2, s, 1)

    def phase1(*bufs):
        for c in load_chunk(0, 0, *bufs):
            c.start()
        for pair in wloads:
            for c in pair:
                c.start()
        pl.semaphore_wait(barrier, 4)

        def body(s, _):
            slot1(bufs, s)
            return ()

        lax.fori_loop(0, n_chunks, body, ())

    pl.run_scoped(phase1, pltpu.VMEM((2, CHUNK, dim), BF), pltpu.VMEM((2, CHUNK, ff), BF), pltpu.VMEM((2, CHUNK, ff), BF))

    base2 = n_chunks * 2

    def slot2(bufs, t):
        q = lax.rem(t, 3)

        @pl.when(t + 2 < n_tiles)
        def _():
            for c in load_col(t + 2, lax.rem(t + 2, 3), *bufs):
                c.start()

        xcol, dycol = bufs
        loads = load_col(t, q, *bufs)
        r = pl.ds(pl.multiple_of(t * TILE, TILE), TILE)
        loads[0].wait()
        loads[1].wait()
        dw = lax.dot_general(xcol[q], dgu[...], TN, preferred_element_type=F32)
        dw = dw.astype(BF)
        for i in range(TILE // 128):
            row = t * TILE + i * 128
            lanes = pl.ds(pl.multiple_of((row // ff) * ff, 128), ff)
            for w in range(2):
                place = pl.ds(pl.multiple_of(starts[w] + row % ff, 128), 128)
                kept[place, lanes] = dw[i * 128:(i + 1) * 128, w * ff:(w + 1) * ff]
        kept[down, r] = lax.dot_general(hidt[...], dycol[q], NN, preferred_element_type=F32).astype(BF)
        run(base2, n_tiles, 1, t, 0)

    def phase2(*bufs):
        for t in range(2):
            for c in load_col(t, t, *bufs):
                c.start()

        def body(t, _):
            slot2(bufs, t)
            return ()

        lax.fori_loop(0, n_tiles, body, ())

    pl.run_scoped(phase2, pltpu.VMEM((3, rows, TILE), BF), pltpu.VMEM((3, rows, TILE), BF))

    rest = sorted((p, PRIO.index(stage), stage, k) for stage in range(1, 8) for k, p in enumerate(POINTS[stage - 1])
                  if p >= base2 + n_tiles)
    for _, _, stage, k in rest:
        stages[stage](k)

    def finish(k, _):
        await_bytes(DG, k, rsem)
        for stage in (AG3, AG2, AG1, DG):
            await_bytes(stage, k, ssem)

        @pl.when(k >= n_chunks - SLOTS)
        def _():
            for stage in (RS1, RS2, RS3):
                await_bytes(stage, k, ssem)

        return ()

    lax.fori_loop(0, n_chunks, finish, ())


def writer(kept, dx, dwg, dwu, dwd, sem):
    rows, (dim, ff) = dx.shape[0], dwg.shape
    pairs = [(kept.at[i * 256:(i + 1) * 256], dx.at[i * 256:(i + 1) * 256]) for i in range(rows // 256)]
    pairs += [(kept.at[rows + i * 128:rows + (i + 1) * 128], dwd.at[i * 128:(i + 1) * 128]) for i in range(ff // 128)]
    for w, out in enumerate((dwg, dwu)):
        start = rows + (1 + w) * ff
        pairs += [(kept.at[start:start + ff, b * ff:(b + 1) * ff], out.at[b * ff:(b + 1) * ff]) for b in range(dim // ff)]
    copies = [pltpu.make_async_copy(a, b, sem.at[i]) for i, (a, b) in enumerate(pairs)]
    for c in copies:
        c.start()
    for c in copies:
        c.wait()


def backward(x, dy, gate, up, w_gate, w_up, w_down):
    rows, dim = x.shape
    ff = gate.shape[1]
    n_chunks, n_blocks = rows // CHUNK, dim // ff
    hbm, inside = pl.BlockSpec(memory_space=pl.ANY), pl.BlockSpec(memory_space=pltpu.VMEM)
    vmem, dma = pltpu.VMEM, pltpu.SemaphoreType.DMA
    kept = pl.pallas_call(
        kernel,
        out_shape=vmem((rows + 3 * ff, dim), BF),
        in_specs=[hbm] * 7,
        out_specs=inside,
        scratch_shapes=[
            vmem((rows, 2 * ff), BF), vmem((ff, rows), BF), vmem((HALF, dim), BF), vmem((HALF, dim), F32),
            vmem((SLOTS, HALF // 8 * 7, dim), BF), vmem((SLOTS, HALF // 2, dim), F32),
            dma((2 * n_blocks + 1,)), dma((3, 2)), dma((2, 3)), pltpu.SemaphoreType.REGULAR,
            dma((8, n_chunks)), dma((8, n_chunks)),
        ],
        compiler_params=pltpu.CompilerParams(collective_id=0, has_side_effects=True, vmem_limit_bytes=VMEM_LIMIT),
        name="mlp_backward",
    )(x, dy, gate, up, w_gate, w_up, w_down)
    return pl.pallas_call(
        writer,
        out_shape=tuple(jax.ShapeDtypeStruct(g, BF) for g in ((rows, dim), (dim, ff), (dim, ff), (ff, dim))),
        in_specs=[inside],
        out_specs=(hbm,) * 4,
        scratch_shapes=[dma((2 * n_blocks + rows // 256 + ff // 128,))],
        compiler_params=pltpu.CompilerParams(vmem_limit_bytes=WRITER_LIMIT),
        name="writer",
    )(kept)


def solution(mesh):
    tokens, columns, rows = P("dp", None), P(None, "tp"), P("tp", None)
    return jax.shard_map(
        backward,
        mesh=mesh,
        in_specs=(tokens, tokens, P("dp", "tp"), P("dp", "tp"), columns, columns, rows),
        out_specs=(tokens, P("dp", "tp"), P("dp", "tp"), P(("dp", "tp"), None)),
        check_vma=False,
    )
```
